256 devices in a mesh: seq: 64 (over x, y, z_lo), head: 4 (over z_hi, core).
Axes of the slice: x: 4, y: 4, z: 8 (z_hi: 2, z_lo: 4; z = z_hi * 4 + z_lo), core: 2. Of those that a mesh axis runs over, the one named last changes fastest.
Arguments:
- prompt_token_query: bfloat16 [2048, 8192], P('seq', 'head'), may hold values from -6 to 6
- prompt_token_key: bfloat16 [2048, 1024], P('seq', 'head'), may hold values from -6 to 6
- prompt_token_value: bfloat16 [2048, 1024], P('seq', 'head'), may hold values from -6 to 6
- response_query_slots: bfloat16 [12288, 8192], P('seq', 'head'), may hold values from -160 to 160
- response_key_slots: bfloat16 [12288, 1024], P('seq', 'head'), may hold values from -6 to 6
- response_value_slots: bfloat16 [12288, 1024], P('seq', 'head'), may hold values from -6 to 6
- lengths: int32 [16], replicated, may hold values from 1 to 32, 64 in all
- block_table: int32 [64], replicated, may hold values from 0 to 63, each once
Outputs:
- prompt_out: bfloat16 [2048, 8192], P(('seq', 'head'))
- answer_out: bfloat16 [12288, 8192], P(('seq', 'head'))
The draws below stay inside these ranges and needn't reach their ends.
Inputs may be any that keep to these rules, and one draw needn't show every extreme that they name: `lengths`: they sum to 64; the largest is exactly 32. `block_table`: A permutation of 0 to 63.
All inputs are finite; a program needn't handle non-finite values.
Results may differ from the reference program's by a relative error of at most 0.007.
Values may be sent and summed in bfloat16 or wider, within the bound.
A program may use at most 64 MiB of HBM per device.

```python
import math
import jax
import jax.numpy as jnp
import numpy as np
from jax import lax

QUERY_HEADS = 64
KEY_VALUE_HEADS = 8
HEAD_SIZE = 128
RESPONSE_BLOCK = 192
PROMPT_PER_SEQ = 32
MEMBERS = 16
RESPONSE_COUNT = 64
LONGEST_BLOCKS = 32
PROMPT_TOKENS = 2048
RESPONSE_TOKENS = 12288
N_SEQ = 64


def paired_keys(key):
    regular_portion = jnp.clip(jax.random.normal(jax.random.fold_in(key, 7001), (PROMPT_TOKENS, KEY_VALUE_HEADS, HEAD_SIZE), jnp.float32), -6.0, 6.0)
    return regular_portion


def draw_prompt_token_key(key, part):
    key_lookup_table = paired_keys(key)
    return key_lookup_table.reshape(PROMPT_TOKENS, KEY_VALUE_HEADS * HEAD_SIZE).astype(jnp.bfloat16)


def draw_response_query_slots(key, part):
    regular_portion = jnp.clip(jax.random.normal(jax.random.fold_in(key, 7003), (RESPONSE_TOKENS, QUERY_HEADS, HEAD_SIZE), jnp.float32), -6.0, 6.0)
    return regular_portion.reshape(RESPONSE_TOKENS, QUERY_HEADS * HEAD_SIZE).astype(jnp.bfloat16)


def shard_levels(key, shape, shards, smallest, high):
    def one(dim, parts):
        steps = jax.random.uniform(jax.random.fold_in(jax.random.fold_in(key, 6), dim), (parts,), jnp.float32, smallest / len(shards), high / len(shards))
        return jnp.repeat(jnp.exp(steps), shape[dim] // parts).reshape((-1,) + (1,) * (len(shape) - dim - 1))

    loudness = one(*shards[0])
    for cut in shards[1:]:
        loudness = loudness * one(*cut)
    return loudness


def length_profile(count, total, most, skew):
    portions = [(1 << 20) // math.isqrt(grade ** skew) + 1 for grade in range(2, count + 1)]
    surplus, given = total - most - (count - 1), [1] * (count - 1)
    while surplus > 0:
        candidates = [i for i in range(count - 1) if given[i] < most]
        whole, budget = sum([portions[i] for i in candidates]), surplus
        for i in candidates:
            extra = min(most - given[i], max(1, budget * portions[i] // whole), surplus)
            given[i] = given[i] + extra
            surplus = surplus - extra
    return np.array([most] + given)


def ragged_sizes(stream_key, amount, total, most, slope):
    if amount == 2:
        one = jax.random.randint(stream_key, (), max(1, total - most), min(most, total - 1) + 1)
        return jnp.stack([one, total - one])
    tallies = jnp.asarray(length_profile(amount, total, most, slope), jnp.int32)
    twos = (amount - 1) // 2
    donor, sink = tallies[1:1 + 2 * twos:2], tallies[2:2 + 2 * twos:2]
    margin = jnp.minimum(donor - 1, most - sink)
    shifted = jax.random.randint(jax.random.fold_in(stream_key, 1), (twos,), 0, 1 << 20) % (margin + 1)
    tallies = tallies.at[1:1 + 2 * twos:2].set(donor - shifted).at[2:2 + 2 * twos:2].set(sink + shifted)
    return tallies[jax.random.permutation(jax.random.fold_in(stream_key, 2), amount)]


def gaussian(rng, shape, deviation, limit, cuts=(), held_as=jnp.bfloat16):
    values = jax.random.normal(rng, shape, jnp.float32) * deviation
    if len(cuts) > 0:
        values = shard_levels(rng, shape, cuts, -0.22, 0.18) * values
    return jnp.clip(values, min=-limit, max=limit).astype(held_as)


def setup_inputs(seed: int = 0) -> dict:
    streams_of = jax.random.split(jax.random.key(seed), 9)
    return {
        "prompt_token_query": gaussian(streams_of[0], (PROMPT_TOKENS, QUERY_HEADS * HEAD_SIZE), 1.0, 6.0, ((0, 64), (1, 4))),
        "prompt_token_key": draw_prompt_token_key(jax.random.fold_in(streams_of[8], 71), 0),
        "prompt_token_value": gaussian(streams_of[2], (PROMPT_TOKENS, KEY_VALUE_HEADS * HEAD_SIZE), 1.0, 6.0, ((0, 64), (1, 4))),
        "response_query_slots": draw_response_query_slots(jax.random.fold_in(streams_of[8], 71), 0),
        "response_key_slots": gaussian(streams_of[4], (RESPONSE_TOKENS, KEY_VALUE_HEADS * HEAD_SIZE), 1.0, 6.0, ((0, 64), (1, 4))),
        "response_value_slots": gaussian(streams_of[5], (RESPONSE_TOKENS, KEY_VALUE_HEADS * HEAD_SIZE), 1.0, 6.0, ((0, 64), (1, 4))),
        "lengths": ragged_sizes(streams_of[6], MEMBERS, RESPONSE_COUNT, LONGEST_BLOCKS, 2).astype(jnp.int32),
        "block_table": jax.random.permutation(streams_of[7], RESPONSE_COUNT).astype(jnp.int32),
    }


def block_roles(lengths, global_blocks):
    bounds = jnp.cumsum(lengths).astype(jnp.int32)
    member = jnp.sum((global_blocks[:, None] >= bounds[None, :]).astype(jnp.int32), axis=1).astype(jnp.int32)
    starts = (bounds - lengths).astype(jnp.int32)
    owner_match = member[:, None] == jnp.arange(lengths.shape[0], dtype=jnp.int32)[None, :]
    first_block = jnp.sum(jnp.where(owner_match, starts[None, :], 0), axis=1).astype(jnp.int32)
    return member, (global_blocks - first_block).astype(jnp.int32), first_block


def attend(query_matrix, key_rows, value_rows, visible):
    scores = jnp.einsum("rjgd,sjd->rjgs", query_matrix.astype(jnp.float32), key_rows.astype(jnp.float32)) * (HEAD_SIZE ** -0.5)
    seen = visible[:, None, None, :]
    masked = jnp.where(seen, scores, -jnp.inf)
    peak_value = jnp.max(masked, axis=-1, keepdims=True)
    weights = jnp.where(seen, jnp.exp(scores - peak_value), 0.0)
    weight_total = jnp.sum(weights, axis=-1)
    rounded = weights.astype(jnp.bfloat16).astype(jnp.float32)
    mixed_sum = jnp.einsum("rjgs,sjd->rjgd", rounded, value_rows.astype(jnp.float32))
    return (mixed_sum / weight_total[..., None]).astype(jnp.bfloat16)


def reference(prompt_token_query, prompt_token_key, prompt_token_value, response_query_slots, response_key_slots, response_value_slots, lengths, block_table):
    query_group_width = QUERY_HEADS // KEY_VALUE_HEADS
    shared_prompt_keys = prompt_token_key.reshape(PROMPT_TOKENS, KEY_VALUE_HEADS, HEAD_SIZE)
    shared_prompt_values = prompt_token_value.reshape(PROMPT_TOKENS, KEY_VALUE_HEADS, HEAD_SIZE)

    def prompt_block(leading_row):
        query_matrix = lax.dynamic_slice_in_dim(prompt_token_query, leading_row, PROMPT_PER_SEQ, 0).reshape(PROMPT_PER_SEQ, KEY_VALUE_HEADS, query_group_width, HEAD_SIZE)
        query_positions = leading_row + jnp.arange(PROMPT_PER_SEQ, dtype=jnp.int32)
        visible = jnp.arange(PROMPT_TOKENS, dtype=jnp.int32)[None, :] <= query_positions[:, None]
        return attend(query_matrix, shared_prompt_keys, shared_prompt_values, visible).reshape(PROMPT_PER_SEQ, QUERY_HEADS * HEAD_SIZE)

    prompt_out = lax.map(prompt_block, jnp.arange(N_SEQ, dtype=jnp.int32) * PROMPT_PER_SEQ).reshape(PROMPT_TOKENS, QUERY_HEADS * HEAD_SIZE)

    inverse = jnp.argsort(block_table).astype(jnp.int32)
    blocked_keys = response_key_slots.reshape(RESPONSE_COUNT, RESPONSE_BLOCK, KEY_VALUE_HEADS, HEAD_SIZE)
    blocked_values = response_value_slots.reshape(RESPONSE_COUNT, RESPONSE_BLOCK, KEY_VALUE_HEADS, HEAD_SIZE)
    member, position, first_block = block_roles(lengths, block_table)

    def answer_block(slot_ordinal):
        query_matrix = lax.dynamic_slice_in_dim(response_query_slots, slot_ordinal * RESPONSE_BLOCK, RESPONSE_BLOCK, 0).reshape(RESPONSE_BLOCK, KEY_VALUE_HEADS, query_group_width, HEAD_SIZE)
        own_position = position[slot_ordinal]
        span = jnp.minimum(first_block[slot_ordinal] + jnp.arange(LONGEST_BLOCKS, dtype=jnp.int32), RESPONSE_COUNT - 1)
        window_slots = inverse[span]
        window_keys = blocked_keys[window_slots].reshape(LONGEST_BLOCKS * RESPONSE_BLOCK, KEY_VALUE_HEADS, HEAD_SIZE)
        window_values = blocked_values[window_slots].reshape(LONGEST_BLOCKS * RESPONSE_BLOCK, KEY_VALUE_HEADS, HEAD_SIZE)
        key_positions = jnp.arange(LONGEST_BLOCKS * RESPONSE_BLOCK, dtype=jnp.int32)
        query_positions = own_position * RESPONSE_BLOCK + jnp.arange(RESPONSE_BLOCK, dtype=jnp.int32)
        own_visible = key_positions[None, :] <= query_positions[:, None]
        visible = jnp.concatenate([jnp.ones((RESPONSE_BLOCK, PROMPT_TOKENS), dtype=bool), own_visible], axis=1)
        all_keys = jnp.concatenate([shared_prompt_keys, window_keys], axis=0)
        all_values = jnp.concatenate([shared_prompt_values, window_values], axis=0)
        return attend(query_matrix, all_keys, all_values, visible).reshape(RESPONSE_BLOCK, QUERY_HEADS * HEAD_SIZE)

    answer_out = lax.map(answer_block, jnp.arange(RESPONSE_COUNT, dtype=jnp.int32)).reshape(RESPONSE_TOKENS, QUERY_HEADS * HEAD_SIZE)
    return prompt_out, answer_out
```

```python
import math

import jax
import jax.numpy as jnp
from jax import lax
from jax.experimental import pallas as pl
from jax.experimental.pallas import tpu as pltpu
from jax.sharding import PartitionSpec as P

bf = jnp.bfloat16
ANY = pl.BlockSpec(memory_space=pl.ANY)
SM = pl.BlockSpec(memory_space=pltpu.SMEM)
VM = pl.BlockSpec(memory_space=pltpu.VMEM)
MESH = pl.DeviceIdType.MESH


def gather_kernel(qr, kr, vr, qp, kp, vp, q_oth, qp_oth, kg, vg, bk, bv,
                  lsem, swap_s, swap_r, z_s, z_r, n_s, n_r, h_s, h_r, N_s, N_r, H_s, H_r, osem):
    s = lax.axis_index("seq")
    x, y, zl = s // 16, (s // 4) % 4, s % 4
    g, par = zl // 2, zl % 2
    base = s - zl
    partner = base + 2 * g + 1 - par
    across = base + 2 * (1 - g) + par

    def dev(dx, dy):
        return {"seq": ((x + dx) % 4) * 16 + ((y + dy) % 4) * 4 + zl}

    ring = {0: (dev(1, 0), dev(3, 0)), 1: (dev(0, 1), dev(0, 3))}

    barrier = pltpu.get_barrier_semaphore()
    for d in ({"seq": partner}, {"seq": across}, *ring[0], *ring[1]):
        pl.semaphore_signal(barrier, inc=1, device_id=d, device_id_type=MESH)
    pl.semaphore_wait(barrier, 6)

    mine = pl.multiple_of(par * 128, 128)
    other = pl.multiple_of((1 - par) * 128, 128)
    wide_other = pl.multiple_of((1 - par) * 1024, 1024)
    bufs = (bk, bv)
    srcs = ((kr, kp), (vr, vp))

    def remote(src, dst, ss, rs, d):
        return pltpu.make_async_remote_copy(src_ref=src, dst_ref=dst, send_sem=ss, recv_sem=rs, device_id=d, device_id_type=MESH)

    sends = []

    def send(src, dst, ss, rs, d):
        c = remote(src, dst, ss, rs, d)
        c.start()
        sends.append(c)

    local = []
    for b in range(2):
        r, p = srcs[b]
        send(r.at[:, pl.ds(other, 128)], bufs[b].at[s, 32:224], swap_s.at[2 * b], swap_r.at[2 * b], {"seq": partner})
        send(p.at[:, pl.ds(other, 128)], bufs[b].at[s, 0:32], swap_s.at[2 * b + 1], swap_r.at[2 * b + 1], {"seq": partner})
        for c in (
            pltpu.make_async_copy(r.at[:, pl.ds(mine, 128)], bufs[b].at[s, 32:224], lsem.at[2 * b]),
            pltpu.make_async_copy(p.at[:, pl.ds(mine, 128)], bufs[b].at[s, 0:32], lsem.at[2 * b + 1]),
        ):
            c.start()
            local.append(c)

    def pair_of(b, dx, dy, gg):
        u = (((x + dx) % 4) * 4 + (y + dy) % 4) * 2 + gg
        return bufs[b].at[pl.ds(2 * u, 2)]

    def half_of(b, dx, dy, gg, e):
        u = (((x + dx) % 4) * 4 + (y + dy) % 4) * 2 + gg
        return bufs[b].at[pl.ds(2 * u + e, 1)]

    outs = (kg, vg)
    puts = []

    def put(b, dx, dy, gg):
        u = (((x + dx) % 4) * 4 + (y + dy) % 4) * 2 + gg
        c = pltpu.make_async_copy(bufs[b].at[pl.ds(2 * u, 2)], outs[b].at[pl.ds(2 * u, 2)], osem.at[b])
        c.start()

    G = (g, 1 - g)

    def off(b, first, second):
        return (second, first) if b == 0 else (first, second)

    def ring1_axis(b):
        return 1 if b == 0 else 0

    def ring1_send(b, w):
        for dirn in range(2):
            blk = pair_of(b, 0, 0, G[w])
            send(blk, blk, n_s.at[b, w, dirn], n_r.at[b, w, dirn], ring[ring1_axis(b)][dirn])

    came = (3, 1)

    def ring1_forward(b, w):
        for dirn in range(2):
            blk = pair_of(b, *off(b, came[dirn], 0), G[w])
            remote(blk, blk, n_s.at[b, w, dirn], n_r.at[b, w, dirn], ring[0][0]).wait_recv()
            hb = half_of(b, *off(b, came[dirn], 0), G[w], dirn)
            send(hb, hb, h_s.at[b, w, dirn], h_r.at[b, w, dirn], ring[ring1_axis(b)][dirn])

    def ring1_halves(b, w):
        for dirn in range(2):
            hb = half_of(b, *off(b, 2, 0), G[w], dirn)
            remote(hb, hb, h_s.at[b, w, dirn], h_r.at[b, w, dirn], ring[0][0]).wait_recv()

    def ring2_send(b, w, first):
        for dirn in range(2):
            blk = pair_of(b, *off(b, first, 0), G[w])
            send(blk, blk, N_s.at[b, w, first, dirn], N_r.at[b, w, first, dirn], ring[1 - ring1_axis(b)][dirn])
        put(b, *off(b, first, 0), G[w])

    def ring2_forward(b, w, first):
        for dirn in range(2):
            blk = pair_of(b, *off(b, first, came[dirn]), G[w])
            remote(blk, blk, N_s.at[b, w, first, dirn], N_r.at[b, w, first, dirn], ring[0][0]).wait_recv()
            hb = half_of(b, *off(b, first, came[dirn]), G[w], dirn)
            send(hb, hb, H_s.at[b, w, first, dirn], H_r.at[b, w, first, dirn], ring[1 - ring1_axis(b)][dirn])
            put(b, *off(b, first, came[dirn]), G[w])

    def ring2_halves(b, w, first):
        for dirn in range(2):
            hb = half_of(b, *off(b, first, 2), G[w], dirn)
            remote(hb, hb, H_s.at[b, w, first, dirn], H_r.at[b, w, first, dirn], ring[0][0]).wait_recv()
        put(b, *off(b, first, 2), G[w])

    for b in range(2):
        for i in range(2):
            local[2 * b + i].wait()
        lo = base + 2 * g + 1 - par
        remote(bufs[b].at[lo, 32:224], bufs[b].at[lo, 32:224], swap_s.at[2 * b], swap_r.at[2 * b], ring[0][0]).wait_recv()
        remote(bufs[b].at[lo, 0:32], bufs[b].at[lo, 0:32], swap_s.at[2 * b + 1], swap_r.at[2 * b + 1], ring[0][0]).wait_recv()
        blk = pair_of(b, 0, 0, g)
        send(blk, blk, z_s.at[b], z_r.at[b], {"seq": across})
        ring1_send(b, 0)
    for b in range(2):
        ring2_send(b, 0, 0)
    send(qr.at[:, pl.ds(wide_other, 1024)], q_oth, swap_s.at[4], swap_r.at[4], {"seq": partner})
    send(qp.at[:, pl.ds(wide_other, 1024)], qp_oth, swap_s.at[5], swap_r.at[5], {"seq": partner})

    for b in range(2):
        ring1_forward(b, 0)
        ring2_send(b, 0, 3)
        ring2_send(b, 0, 1)
    for b in range(2):
        blk = pair_of(b, 0, 0, 1 - g)
        remote(blk, blk, z_s.at[b], z_r.at[b], ring[0][0]).wait_recv()
        ring1_send(b, 1)
        ring2_send(b, 1, 0)
    for b in range(2):
        ring2_forward(b, 0, 0)
    for b in range(2):
        ring1_halves(b, 0)
        ring2_send(b, 0, 2)
    for first in (3, 1):
        for b in range(2):
            ring2_forward(b, 0, first)
    for b in range(2):
        ring1_forward(b, 1)
        ring2_send(b, 1, 3)
        ring2_send(b, 1, 1)
    for b in range(2):
        ring2_forward(b, 1, 0)
    for b in range(2):
        ring1_halves(b, 1)
        ring2_send(b, 1, 2)
    for w, first in ((0, 2), (1, 3), (1, 1), (1, 2)):
        for b in range(2):
            ring2_forward(b, w, first)
    for w in range(2):
        for first in (0, 3, 1, 2):
            for b in range(2):
                ring2_halves(b, w, first)
    remote(q_oth, q_oth, swap_s.at[4], swap_r.at[4], ring[0][0]).wait_recv()
    remote(qp_oth, qp_oth, swap_s.at[5], swap_r.at[5], ring[0][0]).wait_recv()
    for c in sends:
        c.wait_send()
    for b in range(2):
        pltpu.make_async_copy(bufs[b], outs[b], osem.at[b]).wait()


def gather(qr, kr, vr, qp, kp, vp):
    D = pltpu.SemaphoreType.DMA
    return pl.pallas_call(
        gather_kernel,
        out_shape=(
            jax.ShapeDtypeStruct((192, 1024), bf), jax.ShapeDtypeStruct((32, 1024), bf),
            jax.ShapeDtypeStruct((64, 224, 128), bf), jax.ShapeDtypeStruct((64, 224, 128), bf),
        ),
        in_specs=[ANY] * 6,
        out_specs=(ANY,) * 4,
        scratch_shapes=[
            pltpu.VMEM((64, 224, 128), bf), pltpu.VMEM((64, 224, 128), bf),
            D((4,)), D((6,)), D((6,)), D((2,)), D((2,)),
            D((2, 2, 2)), D((2, 2, 2)), D((2, 2, 2)), D((2, 2, 2)),
            D((2, 2, 4, 2)), D((2, 2, 4, 2)), D((2, 2, 4, 2)), D((2, 2, 4, 2)),
            D((2,)),
        ],
        compiler_params=pltpu.CompilerParams(collective_id=0, has_side_effects=True, vmem_limit_bytes=60 * 2**20),
    )(qr, kr, vr, qp, kp, vp)


def exchange_kernel(o_r, o_p, f_p, f_r, lsem, ss, rs):
    s, h = lax.axis_index("seq"), lax.axis_index("head")
    par = s % 2
    partner = s + 1 - 2 * par

    def where(e, dh):
        return {"seq": s if e == 0 else partner, "head": (h + dh) % 4}

    barrier = pltpu.get_barrier_semaphore()
    targets = [(e, dh) for e in range(2) for dh in range(4)][1:]
    for e, dh in targets:
        pl.semaphore_signal(barrier, inc=1, device_id=where(e, dh), device_id_type=MESH)
    pl.semaphore_wait(barrier, 7)

    col = pl.multiple_of((2 * h + par) * 1024, 1024)

    def parts(e, dh):
        pe = par if e == 0 else 1 - par
        to = (h + dh) % 4
        return (
            (o_r.at[pe, pl.ds(pl.multiple_of(48 * to, 16), 48)], f_r.at[:, pl.ds(col, 1024)]),
            (o_p.at[pe, to], f_p.at[:, pl.ds(col, 1024)]),
        )

    def came(e, dh):
        pe = par if e == 0 else 1 - par
        c = pl.multiple_of((2 * ((h - dh + 4) % 4) + pe) * 1024, 1024)
        return f_r.at[:, pl.ds(c, 1024)], f_p.at[:, pl.ds(c, 1024)]

    sends = []
    for e, dh in sorted(targets, key=lambda t: -t[1]):
        for i, (src, dst) in enumerate(parts(e, dh)):
            c = pltpu.make_async_remote_copy(src_ref=src, dst_ref=dst, send_sem=ss.at[e, dh, i], recv_sem=rs.at[e, dh, i], device_id=where(e, dh), device_id_type=MESH)
            c.start()
            sends.append(c)
    loc = [pltpu.make_async_copy(src, dst, lsem.at[i]) for i, (src, dst) in enumerate(parts(0, 0))]
    for c in loc:
        c.start()
    for e, dh in targets:
        for i, dst in enumerate(came(e, dh)):
            pltpu.make_async_remote_copy(src_ref=dst, dst_ref=dst, send_sem=ss.at[e, dh, i], recv_sem=rs.at[e, dh, i], device_id=where(e, dh), device_id_type=MESH).wait_recv()
    for c in sends:
        c.wait_send()
    for c in loc:
        c.wait()


def exchange(o_r, o_p):
    D = pltpu.SemaphoreType.DMA
    return pl.pallas_call(
        exchange_kernel,
        out_shape=(jax.ShapeDtypeStruct((8, 8192), bf), jax.ShapeDtypeStruct((48, 8192), bf)),
        in_specs=[ANY] * 2,
        out_specs=(ANY,) * 2,
        scratch_shapes=[D((2,)), D((2, 4, 2)), D((2, 4, 2))],
        compiler_params=pltpu.CompilerParams(collective_id=1, has_side_effects=True),
    )(o_r, o_p)


C = 128 ** -0.5 * math.log2(math.e)
NEG = -1e30
VROWS = 144
AHEAD = 2

def attn_kernel(meta, lengths, table, q_in, q_oth, qp_in, qp_oth, kg, vg, o_r, o_p,
                qv, qpv, kp, vp, kr, vr, qt, m, acc, inv, sems):
    par = meta[0]
    pair = meta[1]
    c0 = pl.multiple_of(par * 1024, 1024)
    cps = [
        pltpu.make_async_copy(q_in.at[:, pl.ds(c0, 1024)], qv.at[par], sems.at[0]),
        pltpu.make_async_copy(q_oth, qv.at[1 - par], sems.at[1]),
        pltpu.make_async_copy(qp_in.at[:, pl.ds(c0, 1024)], qpv.at[par], sems.at[2]),
        pltpu.make_async_copy(qp_oth, qpv.at[1 - par], sems.at[3]),
        pltpu.make_async_copy(kg.at[:, 0:32, :], kp, sems.at[4]),
        pltpu.make_async_copy(vg.at[:, 0:32, :], vp, sems.at[5]),
        pltpu.make_async_copy(kg.at[:, 32:224, :], kr, sems.at[6]),
        pltpu.make_async_copy(vg.at[:, 32:224, :], vr, sems.at[7]),
    ]
    for cp in cps:
        cp.start()

    def put(i, _):
        inv[table[i]] = i
        return 0
    lax.fori_loop(0, 64, put, 0)

    def locate(e):
        block = table[2 * pair + e]
        def step(i, carry):
            at, first = carry
            first = jnp.where(at <= block, at, first)
            return at + lengths[i], first
        _, first = lax.fori_loop(0, 16, step, (jnp.int32(0), jnp.int32(0)))
        return first, block - first

    for cp in cps[:6]:
        cp.wait()
    m[...] = jnp.full(m.shape, NEG, jnp.float32)
    acc[...] = jnp.zeros(acc.shape, jnp.float32)

    def prep(e, _):
        for i in range(4):
            for j in range(2):
                h = 2 * i + j
                qt[e * 7 + i, :, 128 * j:128 * j + 128] = qv[e, 0:128, 128 * h:128 * h + 128].T
        for i in range(2):
            for j in range(2):
                h = 4 * i + 2 * j
                x = jnp.concatenate([qv[e, 128:192, 128 * h:128 * h + 128], qv[e, 128:192, 128 * h + 128:128 * h + 256]], axis=0)
                qt[e * 7 + 4 + i, :, 128 * j:128 * j + 128] = x.T
        for j in range(2):
            x = jnp.concatenate([qpv[e, :, 128 * h:128 * h + 128] for h in range(4 * j, 4 * j + 4)], axis=0)
            qt[e * 7 + 6, :, 128 * j:128 * j + 128] = x.T
        return 0
    lax.fori_loop(0, 2, prep, 0)

    def absorb_all(ts, k, vt, masks=None):
        n = len(ts)
        m_old = [m[t] for t in ts]
        s = [None] * n
        ps = [None] * n
        def score(i):
            x = jnp.dot(k, qt[ts[i]], preferred_element_type=jnp.float32) * C
            if masks is not None:
                x = jnp.where(masks[i], x, NEG)
            return x
        for i in range(min(AHEAD, n)):
            s[i] = score(i)
        for i in range(n):
            if i + AHEAD < n:
                s[i + AHEAD] = score(i + AHEAD)
            m_new = jnp.maximum(m_old[i], jnp.max(s[i], axis=0, keepdims=True))
            p = jnp.exp2(s[i] - m_new).astype(jnp.bfloat16)
            s[i] = None
            m[ts[i]] = m_new
            acc[ts[i]] = acc[ts[i]] * jnp.exp2(m_old[i] - m_new) + jnp.dot(vt, p, preferred_element_type=jnp.float32)

    def absorb(t, k, vt, mask=None):
        absorb_all([t], k, vt, None if mask is None else [mask])

    def turned(v):
        return jnp.concatenate([v.T, jnp.ones((VROWS - 128, v.shape[0]), jnp.bfloat16)], axis=0)

    def prompt_chunk(i, _):
        k = kp[pl.ds(i * 8, 8)].reshape(256, 128)
        vt = turned(vp[pl.ds(i * 8, 8)].reshape(256, 128))
        absorb_all([e * 7 + t for e in range(2) for t in range(6)], k, vt)
        for e in range(2):
            slot = 2 * pair + e
            @pl.when(i * 8 <= slot)
            def _():
                key = i * 256 + lax.broadcasted_iota(jnp.int32, (256, 256), 0)
                row = slot * 32 + lax.broadcasted_iota(jnp.int32, (256, 256), 1) % 32
                absorb(e * 7 + 6, k, vt, key <= row)
        return 0
    lax.fori_loop(0, 8, prompt_chunk, 0)

    for cp in cps[6:]:
        cp.wait()

    def one_slot(e, _):
        first, pos = locate(e)
        def pair_step(j, _):
            a = inv[first + 2 * j]
            b = inv[first + 2 * j + 1]
            k = jnp.concatenate([kr[a], kr[b]], axis=0)
            vt = turned(jnp.concatenate([vr[a], vr[b]], axis=0))
            absorb_all([e * 7 + t for t in range(6)], k, vt)
            return 0
        lax.fori_loop(0, pos // 2, pair_step, 0)

        @pl.when(pos % 2 == 1)
        def _():
            a = inv[first + pos - 1]
            k = kr[a]
            vt = turned(vr[a])
            absorb_all([e * 7 + t for t in range(6)], k, vt)

        a = inv[first + pos]
        k = kr[a]
        vt = turned(vr[a])
        key = lax.broadcasted_iota(jnp.int32, (192, 256), 0)
        lane = lax.broadcasted_iota(jnp.int32, (192, 256), 1)
        absorb_all([e * 7 + t for t in range(6)], k, vt,
                   [key <= (lane % 128 if t < 4 else 128 + lane % 64) for t in range(6)])
        return 0
    lax.fori_loop(0, 2, one_slot, 0)

    def close(e, _):
        def done(t):
            return (acc[t, 0:128] / acc[t, 128:129]).T.astype(jnp.bfloat16)
        for i in range(4):
            o = done(e * 7 + i)
            for j in range(2):
                h = 2 * i + j
                o_r[e, 0:128, 128 * h:128 * h + 128] = o[128 * j:128 * j + 128]
        for i in range(2):
            o = done(e * 7 + 4 + i)
            for j in range(4):
                h = 4 * i + j
                o_r[e, 128:192, 128 * h:128 * h + 128] = o[64 * j:64 * j + 64]
        o = done(e * 7 + 6)
        for h in range(8):
            o_p[e, :, 128 * h:128 * h + 128] = o[32 * h:32 * h + 32]
        return 0
    lax.fori_loop(0, 2, close, 0)


def attend(meta, lengths, table, q_in, q_oth, qp_in, qp_oth, kg, vg):
    return pl.pallas_call(
        attn_kernel,
        out_shape=(jax.ShapeDtypeStruct((2, 192, 1024), bf), jax.ShapeDtypeStruct((2, 32, 1024), bf)),
        in_specs=[SM] * 3 + [ANY] * 6,
        out_specs=(VM, VM),
        scratch_shapes=[
            pltpu.VMEM((2, 192, 1024), bf), pltpu.VMEM((2, 32, 1024), bf),
            pltpu.VMEM((64, 32, 128), bf), pltpu.VMEM((64, 32, 128), bf),
            pltpu.VMEM((64, 192, 128), bf), pltpu.VMEM((64, 192, 128), bf),
            pltpu.VMEM((14, 128, 256), bf), pltpu.VMEM((14, 1, 256), jnp.float32),
            pltpu.VMEM((14, VROWS, 256), jnp.float32), pltpu.SMEM((64,), jnp.int32),
            pltpu.SemaphoreType.DMA((8,)),
        ],
        compiler_params=pltpu.CompilerParams(vmem_limit_bytes=60 * 2**20),
    )(meta, lengths, table, q_in, q_oth, qp_in, qp_oth, kg, vg)


def on_device(qp, kp, vp, qr, kr, vr, lengths, block_table):
    s = lax.axis_index("seq")
    meta = jnp.stack([s % 2, s // 2]).astype(jnp.int32)
    q_oth, qp_oth, kg, vg = gather(qr, kr, vr, qp, kp, vp)
    o_r, o_p = attend(meta, lengths, block_table, qr, q_oth, qp, qp_oth, kg, vg)
    return exchange(o_r, o_p.reshape(2, 4, 8, 1024))


def solution(mesh):
    split = P("seq", "head")
    out = P(("seq", "head"), None)
    return jax.shard_map(
        on_device, mesh=mesh, in_specs=(split,) * 6 + (P(), P()), out_specs=(out, out), check_vma=False
    )
```

```python
import math

import jax
import jax.numpy as jnp
from jax import lax
from jax.experimental import pallas as pl
from jax.experimental.pallas import tpu as pltpu
from jax.sharding import PartitionSpec as P

bf = jnp.bfloat16
ANY = pl.BlockSpec(memory_space=pl.ANY)
SM = pl.BlockSpec(memory_space=pltpu.SMEM)
VM = pl.BlockSpec(memory_space=pltpu.VMEM)
MESH = pl.DeviceIdType.MESH
C = 128 ** -0.5 * math.log2(math.e)
NEG = -1e30
VROWS = 144


def absorb(qt, m, acc, tiles, k, vt, mask=None):
    n = len(tiles)

    def score(i):
        x = jnp.dot(k, qt[tiles[i]], preferred_element_type=jnp.float32)
        return x if mask is None else jnp.where(mask[i], x, NEG)

    m_old = [m[t] for t in tiles]
    s = [score(0)] + [None] * (n - 1)
    for i in range(n):
        if i + 1 < n:
            s[i + 1] = score(i + 1)
        t = tiles[i]
        m_new = jnp.maximum(m_old[i], jnp.max(s[i], axis=0, keepdims=True))
        p = jnp.exp2(s[i] * C - m_new * C).astype(bf)
        s[i] = None
        m[t] = m_new
        acc[t] = acc[t] * jnp.exp2((m_old[i] - m_new) * C) + jnp.dot(vt, p, preferred_element_type=jnp.float32)


def gather_kernel(qr, kr, vr, qp, kp, vp, qt, m, acc, o_p, kg, vg, bk, bv, bq, bqp, mp, accp, qtp,
                  lsem, swap_s, swap_r, z_s, z_r, n_s, n_r, h_s, h_r, N_s, N_r, H_s, H_r, osem):
    s = lax.axis_index("seq")
    x, y, zl = s // 16, (s // 4) % 4, s % 4
    g, par = zl // 2, zl % 2
    base = s - zl
    partner = base + 2 * g + 1 - par
    across = base + 2 * (1 - g) + par

    def dev(dx, dy):
        return {"seq": ((x + dx) % 4) * 16 + ((y + dy) % 4) * 4 + zl}

    ring = {0: (dev(1, 0), dev(3, 0)), 1: (dev(0, 1), dev(0, 3))}

    barrier = pltpu.get_barrier_semaphore()
    for d in ({"seq": partner}, {"seq": across}, *ring[0], *ring[1]):
        pl.semaphore_signal(barrier, inc=1, device_id=d, device_id_type=MESH)
    pl.semaphore_wait(barrier, 6)

    mine = pl.multiple_of(par * 128, 128)
    other = pl.multiple_of((1 - par) * 128, 128)
    wide_other = pl.multiple_of((1 - par) * 1024, 1024)
    bufs = (bk, bv)
    srcs = ((kr, kp), (vr, vp))

    def remote(src, dst, ss, rs, d):
        return pltpu.make_async_remote_copy(src_ref=src, dst_ref=dst, send_sem=ss, recv_sem=rs, device_id=d, device_id_type=MESH)

    sends = []

    def send(src, dst, ss, rs, d):
        c = remote(src, dst, ss, rs, d)
        c.start()
        sends.append(c)

    local = []
    for b in range(2):
        r, p = srcs[b]
        send(r.at[:, pl.ds(other, 128)], bufs[b].at[s, 32:224], swap_s.at[2 * b], swap_r.at[2 * b], {"seq": partner})
        send(p.at[:, pl.ds(other, 128)], bufs[b].at[s, 0:32], swap_s.at[2 * b + 1], swap_r.at[2 * b + 1], {"seq": partner})
        for c in (
            pltpu.make_async_copy(r.at[:, pl.ds(mine, 128)], bufs[b].at[s, 32:224], lsem.at[2 * b]),
            pltpu.make_async_copy(p.at[:, pl.ds(mine, 128)], bufs[b].at[s, 0:32], lsem.at[2 * b + 1]),
        ):
            c.start()
            local.append(c)

    def pair_of(b, dx, dy, gg):
        u = (((x + dx) % 4) * 4 + (y + dy) % 4) * 2 + gg
        return bufs[b].at[pl.ds(2 * u, 2)]

    def half_of(b, dx, dy, gg, e):
        u = (((x + dx) % 4) * 4 + (y + dy) % 4) * 2 + gg
        return bufs[b].at[pl.ds(2 * u + e, 1)]

    outs = (kg, vg)
    puts = []

    def put(b, dx, dy, gg):
        u = (((x + dx) % 4) * 4 + (y + dy) % 4) * 2 + gg
        pltpu.make_async_copy(bufs[b].at[pl.ds(2 * u, 2), 32:224], outs[b].at[pl.ds(2 * u, 2)], osem.at[b]).start()

    G = (g, 1 - g)

    def off(b, first, second):
        return (second, first) if b == 0 else (first, second)

    def ring1_axis(b):
        return 1 if b == 0 else 0

    def ring1_send(b, w):
        for dirn in range(2):
            blk = pair_of(b, 0, 0, G[w])
            send(blk, blk, n_s.at[b, w, dirn], n_r.at[b, w, dirn], ring[ring1_axis(b)][dirn])

    came = (3, 1)

    def ring1_forward(b, w):
        for dirn in range(2):
            blk = pair_of(b, *off(b, came[dirn], 0), G[w])
            remote(blk, blk, n_s.at[b, w, dirn], n_r.at[b, w, dirn], ring[0][0]).wait_recv()
            hb = half_of(b, *off(b, came[dirn], 0), G[w], dirn)
            send(hb, hb, h_s.at[b, w, dirn], h_r.at[b, w, dirn], ring[ring1_axis(b)][dirn])

    def ring1_halves(b, w):
        for dirn in range(2):
            hb = half_of(b, *off(b, 2, 0), G[w], dirn)
            remote(hb, hb, h_s.at[b, w, dirn], h_r.at[b, w, dirn], ring[0][0]).wait_recv()

    def ring2_send(b, w, first):
        for dirn in range(2):
            blk = pair_of(b, *off(b, first, 0), G[w])
            send(blk, blk, N_s.at[b, w, first, dirn], N_r.at[b, w, first, dirn], ring[1 - ring1_axis(b)][dirn])
        put(b, *off(b, first, 0), G[w])

    def ring2_forward(b, w, first):
        for dirn in range(2):
            blk = pair_of(b, *off(b, first, came[dirn]), G[w])
            remote(blk, blk, N_s.at[b, w, first, dirn], N_r.at[b, w, first, dirn], ring[0][0]).wait_recv()
            hb = half_of(b, *off(b, first, came[dirn]), G[w], dirn)
            send(hb, hb, H_s.at[b, w, first, dirn], H_r.at[b, w, first, dirn], ring[1 - ring1_axis(b)][dirn])
            put(b, *off(b, first, came[dirn]), G[w])

    def ring2_halves(b, w, first):
        for dirn in range(2):
            hb = half_of(b, *off(b, first, 2), G[w], dirn)
            remote(hb, hb, H_s.at[b, w, first, dirn], H_r.at[b, w, first, dirn], ring[0][0]).wait_recv()
        put(b, *off(b, first, 2), G[w])

    for b in range(2):
        for i in range(2):
            local[2 * b + i].wait()
        lo = base + 2 * g + 1 - par
        remote(bufs[b].at[lo, 32:224], bufs[b].at[lo, 32:224], swap_s.at[2 * b], swap_r.at[2 * b], ring[0][0]).wait_recv()
        remote(bufs[b].at[lo, 0:32], bufs[b].at[lo, 0:32], swap_s.at[2 * b + 1], swap_r.at[2 * b + 1], ring[0][0]).wait_recv()
        blk = pair_of(b, 0, 0, g)
        send(blk, blk, z_s.at[b], z_r.at[b], {"seq": across})
        ring1_send(b, 0)
    for b in range(2):
        ring2_send(b, 0, 0)
    wide_mine = pl.multiple_of(par * 1024, 1024)
    qcopies = [
        pltpu.make_async_copy(qr.at[:, pl.ds(wide_mine, 1024)], bq.at[par], lsem.at[4]),
        pltpu.make_async_copy(qp.at[:, pl.ds(wide_mine, 1024)], bqp.at[par], lsem.at[5]),
    ]
    for c in qcopies:
        c.start()
    send(qr.at[:, pl.ds(wide_other, 1024)], bq.at[par], swap_s.at[4], swap_r.at[4], {"seq": partner})
    send(qp.at[:, pl.ds(wide_other, 1024)], bqp.at[par], swap_s.at[5], swap_r.at[5], {"seq": partner})
    m[...] = jnp.full(m.shape, NEG, jnp.float32)
    acc[...] = jnp.zeros(acc.shape, jnp.float32)
    mp[...] = jnp.full(mp.shape, NEG, jnp.float32)
    accp[...] = jnp.zeros(accp.shape, jnp.float32)

    for b in range(2):
        ring1_forward(b, 0)
        ring2_send(b, 0, 3)
        ring2_send(b, 0, 1)
    for b in range(2):
        blk = pair_of(b, 0, 0, 1 - g)
        remote(blk, blk, z_s.at[b], z_r.at[b], ring[0][0]).wait_recv()
        ring1_send(b, 1)
        ring2_send(b, 1, 0)
    for b in range(2):
        ring2_forward(b, 0, 0)
    for b in range(2):
        ring1_halves(b, 0)
        ring2_send(b, 0, 2)
    for c in qcopies:
        c.wait()
    remote(bq.at[1 - par], bq.at[1 - par], swap_s.at[4], swap_r.at[4], ring[0][0]).wait_recv()
    remote(bqp.at[1 - par], bqp.at[1 - par], swap_s.at[5], swap_r.at[5], ring[0][0]).wait_recv()

    def turn_queries(e, _):
        def at(h, lo, hi):
            return bq[e, lo:hi, 128 * h:128 * h + 128]
        for h in range(8):
            qt[e * 6 + h // 2, :, 128 * (h % 2):128 * (h % 2) + 128] = at(h, 0, 128).T
        for j in range(4):
            both = jnp.concatenate([at(2 * j, 128, 192), at(2 * j + 1, 128, 192)], axis=0)
            qt[e * 6 + 4 + j // 2, :, 128 * (j % 2):128 * (j % 2) + 128] = both.T
        for j in range(2):
            rows = jnp.concatenate([bqp[e, :, 128 * h:128 * h + 128] for h in range(4 * j, 4 * j + 4)], axis=0)
            qtp[e, :, 128 * j:128 * j + 128] = rows.T
        return 0
    lax.fori_loop(0, 2, turn_queries, 0)

    key = lax.broadcasted_iota(jnp.int32, (256, 256), 0)
    lane = lax.broadcasted_iota(jnp.int32, (256, 256), 1)
    key_at = (key // 64) * 128 + key % 64
    pair0 = s - par

    def chunk(w, dx):
        plane = (x + dx) % 4

        def rows(ref):
            return jnp.concatenate([ref[pl.ds(plane * 16 + 4 * i + 2 * G[w], 2), 0:32].reshape(64, 128) for i in range(4)], axis=0)
        k = rows(bk)
        vt = jnp.concatenate([rows(bv).T, jnp.ones((VROWS - 128, 256), bf)], axis=0)
        absorb(qt, m, acc, list(range(12)), k, vt)

        @pl.when(plane <= x)
        def _():
            at = key_at + plane * 512 + G[w] * 64
            absorb(qtp, mp, accp, [0, 1], k, vt, [at <= (pair0 + e) * 32 + lane % 32 for e in range(2)])

    def on_both(f, *args):
        for b in range(2):
            f(b, *args)

    on_both(ring2_forward, 0, 3)
    on_both(ring2_forward, 0, 1)
    for b in range(2):
        ring1_forward(b, 1)
        ring2_send(b, 1, 3)
        ring2_send(b, 1, 1)
    on_both(ring2_forward, 0, 2)
    ring2_halves(1, 0, 0)
    chunk(0, 0)
    on_both(ring2_forward, 1, 0)
    on_both(ring1_halves, 1)
    on_both(ring2_send, 1, 2)
    ring2_halves(1, 0, 3)
    chunk(0, 3)
    on_both(ring2_forward, 1, 3)
    ring2_halves(1, 0, 1)
    chunk(0, 1)
    on_both(ring2_forward, 1, 1)
    for first in (0, 3, 1, 2):
        ring2_halves(0, 0, first)
    ring2_halves(1, 0, 2)
    chunk(0, 2)
    on_both(ring2_forward, 1, 2)
    ring2_halves(1, 1, 0)
    chunk(1, 0)
    ring2_halves(1, 1, 3)
    chunk(1, 3)
    ring2_halves(1, 1, 1)
    chunk(1, 1)
    for first in (0, 3, 1, 2):
        ring2_halves(0, 1, first)
    ring2_halves(1, 1, 2)
    chunk(1, 2)
    for e in range(2):
        o = (accp[e, 0:128] / accp[e, 128:129]).T.astype(bf)
        for h in range(8):
            o_p[e, :, 128 * h:128 * h + 128] = o[32 * h:32 * h + 32]
    for c in sends:
        c.wait_send()
    for b in range(2):
        pltpu.make_async_copy(bufs[b].at[:, 32:224], outs[b], osem.at[b]).wait()


def gather(qr, kr, vr, qp, kp, vp):
    D = pltpu.SemaphoreType.DMA
    return pl.pallas_call(
        gather_kernel,
        out_shape=(
            jax.ShapeDtypeStruct((12, 128, 256), bf), jax.ShapeDtypeStruct((12, 1, 256), jnp.float32),
            jax.ShapeDtypeStruct((12, VROWS, 256), jnp.float32), jax.ShapeDtypeStruct((2, 32, 1024), bf),
            jax.ShapeDtypeStruct((64, 192, 128), bf), jax.ShapeDtypeStruct((64, 192, 128), bf),
        ),
        in_specs=[ANY] * 6,
        out_specs=(VM,) * 4 + (ANY,) * 2,
        scratch_shapes=[
            pltpu.VMEM((64, 224, 128), bf), pltpu.VMEM((64, 224, 128), bf),
            pltpu.VMEM((2, 192, 1024), bf), pltpu.VMEM((2, 32, 1024), bf),
            pltpu.VMEM((2, 1, 256), jnp.float32), pltpu.VMEM((2, VROWS, 256), jnp.float32), pltpu.VMEM((2, 128, 256), bf),
            D((6,)), D((6,)), D((6,)), D((2,)), D((2,)),
            D((2, 2, 2)), D((2, 2, 2)), D((2, 2, 2)), D((2, 2, 2)),
            D((2, 2, 4, 2)), D((2, 2, 4, 2)), D((2, 2, 4, 2)), D((2, 2, 4, 2)),
            D((2,)),
        ],
        compiler_params=pltpu.CompilerParams(collective_id=0, has_side_effects=True, vmem_limit_bytes=60 * 2**20),
    )(qr, kr, vr, qp, kp, vp)


def exchange_kernel(o_r, o_p, f_p, f_r, lsem, ss, rs):
    s, h = lax.axis_index("seq"), lax.axis_index("head")
    par = s % 2
    partner = s + 1 - 2 * par

    def where(e, dh):
        return {"seq": s if e == 0 else partner, "head": (h + dh) % 4}

    barrier = pltpu.get_barrier_semaphore()
    targets = [(e, dh) for e in range(2) for dh in range(4)][1:]
    for e, dh in targets:
        pl.semaphore_signal(barrier, inc=1, device_id=where(e, dh), device_id_type=MESH)
    pl.semaphore_wait(barrier, 7)

    col = pl.multiple_of((2 * h + par) * 1024, 1024)

    def parts(e, dh):
        pe = par if e == 0 else 1 - par
        to = (h + dh) % 4
        return (
            (o_r.at[pe, pl.ds(pl.multiple_of(48 * to, 16), 48)], f_r.at[:, pl.ds(col, 1024)]),
            (o_p.at[pe, to], f_p.at[:, pl.ds(col, 1024)]),
        )

    def came(e, dh):
        pe = par if e == 0 else 1 - par
        c = pl.multiple_of((2 * ((h - dh + 4) % 4) + pe) * 1024, 1024)
        return f_r.at[:, pl.ds(c, 1024)], f_p.at[:, pl.ds(c, 1024)]

    sends = []
    for e, dh in sorted(targets, key=lambda t: -t[1]):
        for i, (src, dst) in enumerate(parts(e, dh)):
            c = pltpu.make_async_remote_copy(src_ref=src, dst_ref=dst, send_sem=ss.at[e, dh, i], recv_sem=rs.at[e, dh, i], device_id=where(e, dh), device_id_type=MESH)
            c.start()
            sends.append(c)
    loc = [pltpu.make_async_copy(src, dst, lsem.at[i]) for i, (src, dst) in enumerate(parts(0, 0))]
    for c in loc:
        c.start()
    for e, dh in targets:
        for i, dst in enumerate(came(e, dh)):
            pltpu.make_async_remote_copy(src_ref=dst, dst_ref=dst, send_sem=ss.at[e, dh, i], recv_sem=rs.at[e, dh, i], device_id=where(e, dh), device_id_type=MESH).wait_recv()
    for c in sends:
        c.wait_send()
    for c in loc:
        c.wait()


def exchange(o_r, o_p):
    D = pltpu.SemaphoreType.DMA
    return pl.pallas_call(
        exchange_kernel,
        out_shape=(jax.ShapeDtypeStruct((8, 8192), bf), jax.ShapeDtypeStruct((48, 8192), bf)),
        in_specs=[ANY] * 2,
        out_specs=(ANY,) * 2,
        scratch_shapes=[D((2,)), D((2, 4, 2)), D((2, 4, 2))],
        compiler_params=pltpu.CompilerParams(collective_id=1, has_side_effects=True),
    )(o_r, o_p)


GROUP = 4
KEYS = 192 * GROUP
CHUNK = 256
PARTS = KEYS // CHUNK
TILES = 6


def turned(v):
    return jnp.concatenate([v.T, jnp.ones((VROWS - 128, v.shape[0]), bf)], axis=0)


def stage(qt, m, acc, s_buf, p_buf, a_buf, vt_of, nxt, cur, prev, k_of, mask=None):
    nb, nt = nxt
    cb, ct = cur
    pb, pt = prev
    mc = m[ct] * C
    peak = None
    total = None
    for c in range(PARTS):
        rows = slice(c * CHUNK, (c + 1) * CHUNK)
        x = jnp.dot(k_of(c), qt[nt], preferred_element_type=jnp.float32)
        if mask is not None:
            x = jnp.where(mask(c), x, NEG)
        s_buf[nb, rows] = x
        top = jnp.max(x.reshape(CHUNK // 8, 8, 256), axis=0)
        peak = top if peak is None else jnp.maximum(peak, top)
        p_buf[cb, rows] = jnp.exp2(s_buf[cb, rows] * C - mc).astype(bf)
        o = jnp.dot(vt_of(c), p_buf[pb, rows], preferred_element_type=jnp.float32)
        total = o if total is None else total + o
    m_old = m[nt]
    m_new = jnp.maximum(m_old, jnp.max(peak, axis=0, keepdims=True))
    acc[pt] = acc[pt] * a_buf[pb] + total
    m[nt] = m_new
    a_buf[nb] = jnp.exp2((m_old - m_new) * C)


def attn_kernel(meta, lengths, table, qt_h, m_h, acc_h, kg, vg, o_r, kr, vr, qt, m, acc, s_buf, p_buf, a_buf, vt,
                inv, firsts, lasts, sems):
    pair = meta[0]
    cps = [
        pltpu.make_async_copy(a, b, sems.at[i])
        for i, (a, b) in enumerate(((qt_h, qt), (m_h, m), (acc_h, acc), (kg, kr), (vg, vr)))
    ]
    for cp in cps:
        cp.start()

    def put(i, _):
        inv[table[i]] = i
        return 0
    lax.fori_loop(0, 64, put, 0)

    def note(e, _):
        block = table[2 * pair + e]
        def step(i, carry):
            at, first = carry
            first = jnp.where(at <= block, at, first)
            return at + lengths[i], first
        _, first = lax.fori_loop(0, 16, step, (jnp.int32(0), jnp.int32(0)))
        firsts[e] = first
        lasts[e] = block - first
        return 0
    lax.fori_loop(0, 2, note, 0)

    p_buf[2] = jnp.zeros((KEYS, 256), bf)
    a_buf[2] = jnp.ones((1, 256), jnp.float32)
    vt[...] = jnp.zeros(vt.shape, bf)
    for cp in cps:
        cp.wait()

    def joined(ref, at):
        return jnp.concatenate([ref[inv[jnp.minimum(at + i, 63)]] for i in range(GROUP)], axis=0)

    def part(k):
        return lambda c: k[c * CHUNK:(c + 1) * CHUNK]

    def lanes(v):
        return lambda c: v[:, c * CHUNK:(c + 1) * CHUNK]

    key = lax.broadcasted_iota(jnp.int32, (CHUNK, 256), 0)
    lane = lax.broadcasted_iota(jnp.int32, (CHUNK, 256), 1)

    def masks(t, room):
        row = lane % 128 if t < 4 else 128 + lane % 64
        return lambda c: key + c * CHUNK <= row + room

    def room_of(e, j):
        return (lasts[e] - GROUP * j) * 192

    k0 = part(joined(kr, firsts[0]))
    peak = None
    for c in range(PARTS):
        x = jnp.dot(k0(c), qt[0], preferred_element_type=jnp.float32)
        x = jnp.where(masks(0, room_of(0, 0))(c), x, NEG)
        s_buf[0, c * CHUNK:(c + 1) * CHUNK] = x
        top = jnp.max(x, axis=0, keepdims=True)
        peak = top if peak is None else jnp.maximum(peak, top)
    m_old = m[0]
    m[0] = jnp.maximum(m_old, peak)
    a_buf[0] = jnp.exp2((m_old - m[0]) * C)

    def one_step(e, j, last, then_e, then_j, then_last, before):
        t = e * TILES
        at = firsts[e] + GROUP * j
        k = part(joined(kr, at))
        v = turned(joined(vr, at))
        kn = part(joined(kr, firsts[then_e] + GROUP * then_j))
        for i in range(TILES):
            final = i == TILES - 1
            if final:
                mask = masks(0, room_of(then_e, then_j)) if then_last else None
            else:
                mask = masks(i + 1, room_of(e, j)) if last else None
            stage(
                qt, m, acc, s_buf, p_buf, a_buf,
                lanes(v) if i else (lambda c: vt[:, c * CHUNK:(c + 1) * CHUNK]),
                ((i + 1) % 3, then_e * TILES if final else t + i + 1), (i % 3, t + i),
                ((i + 2) % 3, t + i - 1 if i else before), kn if final else k, mask,
            )
            if i == 0:
                vt[...] = v

    def one_slot(e, before):
        steps = lasts[e] // GROUP

        def full(j, before):
            one_step(e, j, False, e, j + 1, False, before)
            return e * TILES + TILES - 1
        before = lax.fori_loop(0, steps - 1, full, before)

        def last_full(j, before):
            one_step(e, j, False, e, j + 1, True, before)
            return e * TILES + TILES - 1
        before = lax.fori_loop(jnp.maximum(steps - 1, 0), steps, last_full, before)
        one_step(e, steps, True, jnp.minimum(e + 1, 1), 0, True, before)
        return e * TILES + TILES - 1
    lax.fori_loop(0, 2, one_slot, TILES - 1)

    end = 2 * TILES - 1
    acc[end] = acc[end] * a_buf[2] + jnp.dot(vt[...], p_buf[2], preferred_element_type=jnp.float32)

    def close(e, _):
        def done(t):
            return (acc[t, 0:128] / acc[t, 128:129]).T.astype(bf)
        for i in range(4):
            o = done(e * TILES + i)
            for j in range(2):
                h = 2 * i + j
                o_r[e, 0:128, 128 * h:128 * h + 128] = o[128 * j:128 * j + 128]
        for i in range(2):
            o = done(e * TILES + 4 + i)
            for j in range(4):
                h = 4 * i + j
                o_r[e, 128:192, 128 * h:128 * h + 128] = o[64 * j:64 * j + 64]
        return 0
    lax.fori_loop(0, 2, close, 0)


def attend(meta, lengths, table, qt, m, acc, kg, vg):
    return pl.pallas_call(
        attn_kernel,
        out_shape=jax.ShapeDtypeStruct((2, 192, 1024), bf),
        in_specs=[SM] * 3 + [ANY] * 5,
        out_specs=VM,
        scratch_shapes=[
            pltpu.VMEM((64, 192, 128), bf), pltpu.VMEM((64, 192, 128), bf),
            pltpu.VMEM((12, 128, 256), bf), pltpu.VMEM((12, 1, 256), jnp.float32),
            pltpu.VMEM((12, VROWS, 256), jnp.float32),
            pltpu.VMEM((3, KEYS, 256), jnp.float32), pltpu.VMEM((3, KEYS, 256), bf),
            pltpu.VMEM((3, 1, 256), jnp.float32), pltpu.VMEM((VROWS, KEYS), bf),
            pltpu.SMEM((64,), jnp.int32), pltpu.SMEM((4,), jnp.int32), pltpu.SMEM((4,), jnp.int32),
            pltpu.SemaphoreType.DMA((5,)),
        ],
        compiler_params=pltpu.CompilerParams(vmem_limit_bytes=60 * 2**20),
    )(meta, lengths, table, qt, m, acc, kg, vg)


def on_device(qp, kp, vp, qr, kr, vr, lengths, block_table):
    pair = (lax.axis_index("seq") // 2).astype(jnp.int32).reshape(1)
    qt, m, acc, o_p, kg, vg = gather(qr, kr, vr, qp, kp, vp)
    o_r = attend(pair, lengths, block_table, qt, m, acc, kg, vg)
    return exchange(o_r, o_p.reshape(2, 4, 8, 1024))


def solution(mesh):
    split = P("seq", "head")
    out = P(("seq", "head"), None)
    return jax.shard_map(
        on_device, mesh=mesh, in_specs=(split,) * 6 + (P(), P()), out_specs=(out, out), check_vma=False
    )
```

```python
import math

import jax
import jax.numpy as jnp
from jax import lax
from jax.experimental import pallas as pl
from jax.experimental.pallas import tpu as pltpu
from jax.sharding import PartitionSpec as P

bf = jnp.bfloat16
ANY = pl.BlockSpec(memory_space=pl.ANY)
SM = pl.BlockSpec(memory_space=pltpu.SMEM)
VM = pl.BlockSpec(memory_space=pltpu.VMEM)
MESH = pl.DeviceIdType.MESH
C = 128 ** -0.5 * math.log2(math.e)
NEG = -1e30
VROWS = 144


def absorb(qt, m, acc, tiles, k, vt, mask=None):
    n = len(tiles)

    def score(i):
        x = jnp.dot(k, qt[tiles[i]], preferred_element_type=jnp.float32)
        return x if mask is None else jnp.where(mask[i], x, NEG)

    m_old = [m[t] for t in tiles]
    s = [score(0)] + [None] * (n - 1)
    for i in range(n):
        if i + 1 < n:
            s[i + 1] = score(i + 1)
        t = tiles[i]
        m_new = jnp.maximum(m_old[i], jnp.max(s[i], axis=0, keepdims=True))
        p = jnp.exp2(s[i] * C - m_new * C).astype(bf)
        s[i] = None
        m[t] = m_new
        acc[t] = acc[t] * jnp.exp2((m_old[i] - m_new) * C) + jnp.dot(vt, p, preferred_element_type=jnp.float32)


def gather_kernel(qr, kr, vr, qp, kp, vp, qt, m, acc, o_p, kg, vg, bk, bv, bq, bqp, mp, accp, qtp,
                  lsem, swap_s, swap_r, z_s, z_r, n_s, n_r, h_s, h_r, N_s, N_r, H_s, H_r, osem):
    s = lax.axis_index("seq")
    x, y, zl = s // 16, (s // 4) % 4, s % 4
    g, par = zl // 2, zl % 2
    base = s - zl
    partner = base + 2 * g + 1 - par
    across = base + 2 * (1 - g) + par

    def dev(dx, dy):
        return {"seq": ((x + dx) % 4) * 16 + ((y + dy) % 4) * 4 + zl}

    ring = {0: (dev(1, 0), dev(3, 0)), 1: (dev(0, 1), dev(0, 3))}

    barrier = pltpu.get_barrier_semaphore()
    for d in ({"seq": partner}, {"seq": across}, *ring[0], *ring[1]):
        pl.semaphore_signal(barrier, inc=1, device_id=d, device_id_type=MESH)
    pl.semaphore_wait(barrier, 6)

    mine = pl.multiple_of(par * 128, 128)
    other = pl.multiple_of((1 - par) * 128, 128)
    wide_other = pl.multiple_of((1 - par) * 1024, 1024)
    bufs = (bk, bv)
    srcs = ((kr, kp), (vr, vp))

    def remote(src, dst, ss, rs, d):
        return pltpu.make_async_remote_copy(src_ref=src, dst_ref=dst, send_sem=ss, recv_sem=rs, device_id=d, device_id_type=MESH)

    sends = []

    def send(src, dst, ss, rs, d):
        c = remote(src, dst, ss, rs, d)
        c.start()
        sends.append(c)

    local = []
    for b in range(2):
        r, p = srcs[b]
        send(r.at[:, pl.ds(other, 128)], bufs[b].at[s, 32:224], swap_s.at[2 * b], swap_r.at[2 * b], {"seq": partner})
        send(p.at[:, pl.ds(other, 128)], bufs[b].at[s, 0:32], swap_s.at[2 * b + 1], swap_r.at[2 * b + 1], {"seq": partner})
        for c in (
            pltpu.make_async_copy(r.at[:, pl.ds(mine, 128)], bufs[b].at[s, 32:224], lsem.at[2 * b]),
            pltpu.make_async_copy(p.at[:, pl.ds(mine, 128)], bufs[b].at[s, 0:32], lsem.at[2 * b + 1]),
        ):
            c.start()
            local.append(c)

    def pair_of(b, dx, dy, gg):
        u = (((x + dx) % 4) * 4 + (y + dy) % 4) * 2 + gg
        return bufs[b].at[pl.ds(2 * u, 2)]

    def slots_of(dx, dy, gg):
        return ((((x + dx) % 4) * 4 + (y + dy) % 4) * 2 + gg) * 2

    def half_of(b, dx, dy, gg, e):
        u = (((x + dx) % 4) * 4 + (y + dy) % 4) * 2 + gg
        return bufs[b].at[pl.ds(2 * u + e, 1)]

    outs = (kg, vg)
    puts = []

    def put(b, dx, dy, gg):
        u = (((x + dx) % 4) * 4 + (y + dy) % 4) * 2 + gg
        pltpu.make_async_copy(bufs[b].at[pl.ds(2 * u, 2), 32:224], outs[b].at[pl.ds(2 * u, 2)], osem.at[b]).start()

    G = (g, 1 - g)

    def off(b, first, second):
        return (second, first) if b == 0 else (first, second)

    def ring1_axis(b):
        return 1 if b == 0 else 0

    def ring1_send(b, w):
        for dirn in range(2):
            blk = pair_of(b, 0, 0, G[w])
            send(blk, blk, n_s.at[b, w, dirn], n_r.at[b, w, dirn], ring[ring1_axis(b)][dirn])

    came = (3, 1)

    def ring1_forward(b, w):
        for dirn in range(2):
            blk = pair_of(b, *off(b, came[dirn], 0), G[w])
            remote(blk, blk, n_s.at[b, w, dirn], n_r.at[b, w, dirn], ring[0][0]).wait_recv()
            hb = half_of(b, *off(b, came[dirn], 0), G[w], dirn)
            send(hb, hb, h_s.at[b, w, dirn], h_r.at[b, w, dirn], ring[ring1_axis(b)][dirn])

    def ring1_halves(b, w):
        for dirn in range(2):
            hb = half_of(b, *off(b, 2, 0), G[w], dirn)
            remote(hb, hb, h_s.at[b, w, dirn], h_r.at[b, w, dirn], ring[0][0]).wait_recv()

    def ring2_send(b, w, first):
        for dirn in range(2):
            blk = pair_of(b, *off(b, first, 0), G[w])
            send(blk, blk, N_s.at[b, w, first, dirn], N_r.at[b, w, first, dirn], ring[1 - ring1_axis(b)][dirn])
        put(b, *off(b, first, 0), G[w])

    def ring2_forward(b, w, first):
        for dirn in range(2):
            blk = pair_of(b, *off(b, first, came[dirn]), G[w])
            remote(blk, blk, N_s.at[b, w, first, dirn], N_r.at[b, w, first, dirn], ring[0][0]).wait_recv()
            hb = half_of(b, *off(b, first, came[dirn]), G[w], dirn)
            send(hb, hb, H_s.at[b, w, first, dirn], H_r.at[b, w, first, dirn], ring[1 - ring1_axis(b)][dirn])
            put(b, *off(b, first, came[dirn]), G[w])

    def ring2_halves(b, w, first):
        for dirn in range(2):
            hb = half_of(b, *off(b, first, 2), G[w], dirn)
            remote(hb, hb, H_s.at[b, w, first, dirn], H_r.at[b, w, first, dirn], ring[0][0]).wait_recv()
        put(b, *off(b, first, 2), G[w])

    for b in range(2):
        for i in range(2):
            local[2 * b + i].wait()
        lo = base + 2 * g + 1 - par
        remote(bufs[b].at[lo, 32:224], bufs[b].at[lo, 32:224], swap_s.at[2 * b], swap_r.at[2 * b], ring[0][0]).wait_recv()
        remote(bufs[b].at[lo, 0:32], bufs[b].at[lo, 0:32], swap_s.at[2 * b + 1], swap_r.at[2 * b + 1], ring[0][0]).wait_recv()
        blk = pair_of(b, 0, 0, g)
        send(blk, blk, z_s.at[b], z_r.at[b], {"seq": across})
        ring1_send(b, 0)
    for b in range(2):
        ring2_send(b, 0, 0)
    wide_mine = pl.multiple_of(par * 1024, 1024)
    qcopies = [
        pltpu.make_async_copy(qr.at[:, pl.ds(wide_mine, 1024)], bq.at[par], lsem.at[4]),
        pltpu.make_async_copy(qp.at[:, pl.ds(wide_mine, 1024)], bqp.at[par], lsem.at[5]),
    ]
    for c in qcopies:
        c.start()
    send(qr.at[:, pl.ds(wide_other, 1024)], bq.at[par], swap_s.at[4], swap_r.at[4], {"seq": partner})
    send(qp.at[:, pl.ds(wide_other, 1024)], bqp.at[par], swap_s.at[5], swap_r.at[5], {"seq": partner})
    m[...] = jnp.full(m.shape, NEG, jnp.float32)
    acc[...] = jnp.zeros(acc.shape, jnp.float32)
    mp[...] = jnp.full(mp.shape, NEG, jnp.float32)
    accp[...] = jnp.zeros(accp.shape, jnp.float32)

    for b in range(2):
        ring1_forward(b, 0)
        ring2_send(b, 0, 3)
        ring2_send(b, 0, 1)
    for b in range(2):
        blk = pair_of(b, 0, 0, 1 - g)
        remote(blk, blk, z_s.at[b], z_r.at[b], ring[0][0]).wait_recv()
        ring1_send(b, 1)
        ring2_send(b, 1, 0)
    for b in range(2):
        ring2_forward(b, 0, 0)
    for b in range(2):
        ring1_halves(b, 0)
        ring2_send(b, 0, 2)
    for c in qcopies:
        c.wait()
    remote(bq.at[1 - par], bq.at[1 - par], swap_s.at[4], swap_r.at[4], ring[0][0]).wait_recv()
    remote(bqp.at[1 - par], bqp.at[1 - par], swap_s.at[5], swap_r.at[5], ring[0][0]).wait_recv()

    def turn_queries(e, _):
        def at(h, lo, hi):
            return bq[e, lo:hi, 128 * h:128 * h + 128]
        for h in range(8):
            qt[e * 6 + h // 2, :, 128 * (h % 2):128 * (h % 2) + 128] = at(h, 0, 128).T
        for j in range(4):
            both = jnp.concatenate([at(2 * j, 128, 192), at(2 * j + 1, 128, 192)], axis=0)
            qt[e * 6 + 4 + j // 2, :, 128 * (j % 2):128 * (j % 2) + 128] = both.T
        for j in range(2):
            rows = jnp.concatenate([bqp[e, :, 128 * h:128 * h + 128] for h in range(4 * j, 4 * j + 4)], axis=0)
            qtp[e, :, 128 * j:128 * j + 128] = rows.T
        return 0
    lax.fori_loop(0, 2, turn_queries, 0)

    key = lax.broadcasted_iota(jnp.int32, (256, 256), 0)
    lane = lax.broadcasted_iota(jnp.int32, (256, 256), 1)
    pair0 = s - par

    def chunk(w, *where):
        at = [slots_of(dx, dy, G[w]) for dx, dy in where]

        def rows(ref):
            return jnp.concatenate([ref[pl.ds(i, 2), 0:32].reshape(64, 128) for i in at], axis=0)
        k = rows(bk)
        vt = jnp.concatenate([rows(bv).T, jnp.ones((VROWS - 128, 256), bf)], axis=0)
        absorb(qt, m, acc, list(range(12)), k, vt)

        first = jnp.minimum(jnp.minimum(at[0], at[1]), jnp.minimum(at[2], at[3]))

        @pl.when(first <= pair0 + 1)
        def _():
            place = jnp.where(key < 128, jnp.where(key < 64, at[0], at[1]), jnp.where(key < 192, at[2], at[3])) * 32 + key % 64
            absorb(qtp, mp, accp, [0, 1], k, vt, [place <= (pair0 + e) * 32 + lane % 32 for e in range(2)])

    near = ((0, 0), (0, 1), (0, 3), (1, 0))
    corner = ((3, 0), (1, 1), (1, 3), (3, 1))
    far_x = ((2, 0), (2, 1), (2, 3), (2, 2))
    far_y = ((0, 2), (1, 2), (3, 2), (3, 3))

    def on_both(f, *args):
        for b in range(2):
            f(b, *args)

    on_both(ring2_forward, 0, 3)
    on_both(ring2_forward, 0, 1)
    chunk(0, *near)
    for b in range(2):
        ring1_forward(b, 1)
        ring2_send(b, 1, 3)
        ring2_send(b, 1, 1)
    on_both(ring2_forward, 0, 2)
    chunk(0, *corner)
    on_both(ring2_forward, 1, 0)
    on_both(ring1_halves, 1)
    on_both(ring2_send, 1, 2)
    for first in (0, 3, 1):
        ring2_halves(1, 0, first)
    chunk(0, *far_y)
    on_both(ring2_forward, 1, 3)
    on_both(ring2_forward, 1, 1)
    chunk(1, *near)
    on_both(ring2_forward, 1, 2)
    ring2_halves(1, 0, 2)
    for first in (0, 3, 1, 2):
        ring2_halves(0, 0, first)
    chunk(0, *far_x)
    chunk(1, *corner)
    for first in (0, 3, 1):
        ring2_halves(1, 1, first)
    chunk(1, *far_y)
    ring2_halves(1, 1, 2)
    for first in (0, 3, 1, 2):
        ring2_halves(0, 1, first)
    chunk(1, *far_x)
    for e in range(2):
        o = (accp[e, 0:128] / accp[e, 128:129]).T.astype(bf)
        for h in range(8):
            o_p[e, :, 128 * h:128 * h + 128] = o[32 * h:32 * h + 32]
    for c in sends:
        c.wait_send()
    for b in range(2):
        pltpu.make_async_copy(bufs[b].at[:, 32:224], outs[b], osem.at[b]).wait()


def gather(qr, kr, vr, qp, kp, vp):
    D = pltpu.SemaphoreType.DMA
    return pl.pallas_call(
        gather_kernel,
        out_shape=(
            jax.ShapeDtypeStruct((12, 128, 256), bf), jax.ShapeDtypeStruct((12, 1, 256), jnp.float32),
            jax.ShapeDtypeStruct((12, VROWS, 256), jnp.float32), jax.ShapeDtypeStruct((2, 32, 1024), bf),
            jax.ShapeDtypeStruct((64, 192, 128), bf), jax.ShapeDtypeStruct((64, 192, 128), bf),
        ),
        in_specs=[ANY] * 6,
        out_specs=(VM,) * 4 + (ANY,) * 2,
        scratch_shapes=[
            pltpu.VMEM((64, 224, 128), bf), pltpu.VMEM((64, 224, 128), bf),
            pltpu.VMEM((2, 192, 1024), bf), pltpu.VMEM((2, 32, 1024), bf),
            pltpu.VMEM((2, 1, 256), jnp.float32), pltpu.VMEM((2, VROWS, 256), jnp.float32), pltpu.VMEM((2, 128, 256), bf),
            D((6,)), D((6,)), D((6,)), D((2,)), D((2,)),
            D((2, 2, 2)), D((2, 2, 2)), D((2, 2, 2)), D((2, 2, 2)),
            D((2, 2, 4, 2)), D((2, 2, 4, 2)), D((2, 2, 4, 2)), D((2, 2, 4, 2)),
            D((2,)),
        ],
        compiler_params=pltpu.CompilerParams(collective_id=0, has_side_effects=True, vmem_limit_bytes=60 * 2**20),
    )(qr, kr, vr, qp, kp, vp)


def exchange_kernel(o_r, o_p, f_p, f_r, lsem, ss, rs):
    s, h = lax.axis_index("seq"), lax.axis_index("head")
    par = s % 2
    partner = s + 1 - 2 * par

    def where(e, dh):
        return {"seq": s if e == 0 else partner, "head": (h + dh) % 4}

    barrier = pltpu.get_barrier_semaphore()
    targets = [(e, dh) for e in range(2) for dh in range(4)][1:]
    for e, dh in targets:
        pl.semaphore_signal(barrier, inc=1, device_id=where(e, dh), device_id_type=MESH)
    pl.semaphore_wait(barrier, 7)

    col = pl.multiple_of((2 * h + par) * 1024, 1024)

    def parts(e, dh):
        pe = par if e == 0 else 1 - par
        to = (h + dh) % 4
        return (
            (o_r.at[pe, pl.ds(pl.multiple_of(48 * to, 16), 48)], f_r.at[:, pl.ds(col, 1024)]),
            (o_p.at[pe, to], f_p.at[:, pl.ds(col, 1024)]),
        )

    def came(e, dh):
        pe = par if e == 0 else 1 - par
        c = pl.multiple_of((2 * ((h - dh + 4) % 4) + pe) * 1024, 1024)
        return f_r.at[:, pl.ds(c, 1024)], f_p.at[:, pl.ds(c, 1024)]

    sends = []
    for e, dh in sorted(targets, key=lambda t: -t[1]):
        for i, (src, dst) in enumerate(parts(e, dh)):
            c = pltpu.make_async_remote_copy(src_ref=src, dst_ref=dst, send_sem=ss.at[e, dh, i], recv_sem=rs.at[e, dh, i], device_id=where(e, dh), device_id_type=MESH)
            c.start()
            sends.append(c)
    loc = [pltpu.make_async_copy(src, dst, lsem.at[i]) for i, (src, dst) in enumerate(parts(0, 0))]
    for c in loc:
        c.start()
    for e, dh in targets:
        for i, dst in enumerate(came(e, dh)):
            pltpu.make_async_remote_copy(src_ref=dst, dst_ref=dst, send_sem=ss.at[e, dh, i], recv_sem=rs.at[e, dh, i], device_id=where(e, dh), device_id_type=MESH).wait_recv()
    for c in sends:
        c.wait_send()
    for c in loc:
        c.wait()


def exchange(o_r, o_p):
    D = pltpu.SemaphoreType.DMA
    return pl.pallas_call(
        exchange_kernel,
        out_shape=(jax.ShapeDtypeStruct((8, 8192), bf), jax.ShapeDtypeStruct((48, 8192), bf)),
        in_specs=[ANY] * 2,
        out_specs=(ANY,) * 2,
        scratch_shapes=[D((2,)), D((2, 4, 2)), D((2, 4, 2))],
        compiler_params=pltpu.CompilerParams(collective_id=1, has_side_effects=True),
    )(o_r, o_p)


def settle_kernel(a, b, c, d):
    c[...] = a[...]
    d[...] = b[...]


def settle(a, b):
    return pl.pallas_call(
        settle_kernel,
        out_shape=(jax.ShapeDtypeStruct(a.shape, a.dtype), jax.ShapeDtypeStruct(b.shape, b.dtype)),
        in_specs=[VM] * 2,
        out_specs=(VM,) * 2,
    )(a, b)


GROUP = 4
KEYS = 192 * GROUP
CHUNK = 256
PARTS = KEYS // CHUNK
TILES = 6


def turned(v):
    return jnp.concatenate([v.T, jnp.ones((VROWS - 128, v.shape[0]), bf)], axis=0)


def stage(qt, m, acc, s_buf, p_buf, a_buf, vt_of, nxt, cur, prev, k_of, mask=None):
    nb, nt = nxt
    cb, ct = cur
    pb, pt = prev
    mc = m[ct] * C
    peak = None
    total = None
    for c in range(PARTS):
        rows = slice(c * CHUNK, (c + 1) * CHUNK)
        x = jnp.dot(k_of(c), qt[nt], preferred_element_type=jnp.float32)
        if mask is not None:
            x = jnp.where(mask(c), x, NEG)
        s_buf[nb, rows] = x
        top = jnp.max(x.reshape(CHUNK // 8, 8, 256), axis=0)
        peak = top if peak is None else jnp.maximum(peak, top)
        p_buf[cb, rows] = jnp.exp2(s_buf[cb, rows] * C - mc).astype(bf)
        o = jnp.dot(vt_of(c), p_buf[pb, rows], preferred_element_type=jnp.float32)
        total = o if total is None else total + o
    m_old = m[nt]
    m_new = jnp.maximum(m_old, jnp.max(peak, axis=0, keepdims=True))
    acc[pt] = acc[pt] * a_buf[pb] + total
    m[nt] = m_new
    a_buf[nb] = jnp.exp2((m_old - m_new) * C)


def attn_kernel(meta, lengths, table, qt_h, m_h, acc_h, kg, vg, o_r, kr, vr, qt, m, acc, s_buf, p_buf, a_buf, vt,
                inv, firsts, lasts, sems):
    pair = meta[0]
    cps = [
        pltpu.make_async_copy(a, b, sems.at[i])
        for i, (a, b) in enumerate(((qt_h, qt), (m_h, m), (acc_h, acc), (kg, kr), (vg, vr)))
    ]
    for cp in cps:
        cp.start()

    def put(i, _):
        inv[table[i]] = i
        return 0
    lax.fori_loop(0, 64, put, 0)

    def note(e, _):
        block = table[2 * pair + e]
        def step(i, carry):
            at, first = carry
            first = jnp.where(at <= block, at, first)
            return at + lengths[i], first
        _, first = lax.fori_loop(0, 16, step, (jnp.int32(0), jnp.int32(0)))
        firsts[e] = first
        lasts[e] = block - first
        return 0
    lax.fori_loop(0, 2, note, 0)

    p_buf[2] = jnp.zeros((KEYS, 256), bf)
    a_buf[2] = jnp.ones((1, 256), jnp.float32)
    vt[...] = jnp.zeros(vt.shape, bf)
    for cp in cps:
        cp.wait()

    def joined(ref, at):
        return jnp.concatenate([ref[inv[jnp.minimum(at + i, 63)]] for i in range(GROUP)], axis=0)

    def part(k):
        return lambda c: k[c * CHUNK:(c + 1) * CHUNK]

    def lanes(v):
        return lambda c: v[:, c * CHUNK:(c + 1) * CHUNK]

    key = lax.broadcasted_iota(jnp.int32, (CHUNK, 256), 0)
    lane = lax.broadcasted_iota(jnp.int32, (CHUNK, 256), 1)

    def masks(t, room):
        row = lane % 128 if t < 4 else 128 + lane % 64
        return lambda c: key + c * CHUNK <= row + room

    def room_of(e, j):
        return (lasts[e] - GROUP * j) * 192

    k0 = part(joined(kr, firsts[0]))
    peak = None
    for c in range(PARTS):
        x = jnp.dot(k0(c), qt[0], preferred_element_type=jnp.float32)
        x = jnp.where(masks(0, room_of(0, 0))(c), x, NEG)
        s_buf[0, c * CHUNK:(c + 1) * CHUNK] = x
        top = jnp.max(x, axis=0, keepdims=True)
        peak = top if peak is None else jnp.maximum(peak, top)
    m_old = m[0]
    m[0] = jnp.maximum(m_old, peak)
    a_buf[0] = jnp.exp2((m_old - m[0]) * C)

    def one_step(e, j, last, then_e, then_j, then_last, before):
        t = e * TILES
        at = firsts[e] + GROUP * j
        k = part(joined(kr, at))
        v = turned(joined(vr, at))
        kn = part(joined(kr, firsts[then_e] + GROUP * then_j))
        for i in range(TILES):
            final = i == TILES - 1
            if final:
                mask = masks(0, room_of(then_e, then_j)) if then_last else None
            else:
                mask = masks(i + 1, room_of(e, j)) if last else None
            stage(
                qt, m, acc, s_buf, p_buf, a_buf,
                lanes(v) if i else (lambda c: vt[:, c * CHUNK:(c + 1) * CHUNK]),
                ((i + 1) % 3, then_e * TILES if final else t + i + 1), (i % 3, t + i),
                ((i + 2) % 3, t + i - 1 if i else before), kn if final else k, mask,
            )
            if i == 0:
                vt[...] = v

    def one_slot(e, before):
        steps = lasts[e] // GROUP

        def full(j, before):
            one_step(e, j, False, e, j + 1, False, before)
            return e * TILES + TILES - 1
        before = lax.fori_loop(0, steps - 1, full, before)

        def last_full(j, before):
            one_step(e, j, False, e, j + 1, True, before)
            return e * TILES + TILES - 1
        before = lax.fori_loop(jnp.maximum(steps - 1, 0), steps, last_full, before)
        one_step(e, steps, True, jnp.minimum(e + 1, 1), 0, True, before)
        return e * TILES + TILES - 1
    lax.fori_loop(0, 2, one_slot, TILES - 1)

    end = 2 * TILES - 1
    acc[end] = acc[end] * a_buf[2] + jnp.dot(vt[...], p_buf[2], preferred_element_type=jnp.float32)

    def close(e, _):
        def done(t):
            return (acc[t, 0:128] / acc[t, 128:129]).T.astype(bf)
        for i in range(4):
            o = done(e * TILES + i)
            for j in range(2):
                h = 2 * i + j
                o_r[e, 0:128, 128 * h:128 * h + 128] = o[128 * j:128 * j + 128]
        for i in range(2):
            o = done(e * TILES + 4 + i)
            for j in range(4):
                h = 4 * i + j
                o_r[e, 128:192, 128 * h:128 * h + 128] = o[64 * j:64 * j + 64]
        return 0
    lax.fori_loop(0, 2, close, 0)


def attend(meta, lengths, table, qt, m, acc, kg, vg):
    return pl.pallas_call(
        attn_kernel,
        out_shape=jax.ShapeDtypeStruct((2, 192, 1024), bf),
        in_specs=[SM] * 3 + [ANY] * 5,
        out_specs=VM,
        scratch_shapes=[
            pltpu.VMEM((64, 192, 128), bf), pltpu.VMEM((64, 192, 128), bf),
            pltpu.VMEM((12, 128, 256), bf), pltpu.VMEM((12, 1, 256), jnp.float32),
            pltpu.VMEM((12, VROWS, 256), jnp.float32),
            pltpu.VMEM((3, KEYS, 256), jnp.float32), pltpu.VMEM((3, KEYS, 256), bf),
            pltpu.VMEM((3, 1, 256), jnp.float32), pltpu.VMEM((VROWS, KEYS), bf),
            pltpu.SMEM((64,), jnp.int32), pltpu.SMEM((4,), jnp.int32), pltpu.SMEM((4,), jnp.int32),
            pltpu.SemaphoreType.DMA((5,)),
        ],
        compiler_params=pltpu.CompilerParams(vmem_limit_bytes=60 * 2**20),
    )(meta, lengths, table, qt, m, acc, kg, vg)


def on_device(qp, kp, vp, qr, kr, vr, lengths, block_table):
    pair = (lax.axis_index("seq") // 2).astype(jnp.int32).reshape(1)
    qt, m, acc, o_p, kg, vg = gather(qr, kr, vr, qp, kp, vp)
    o_r = attend(pair, lengths, block_table, qt, m, acc, kg, vg)
    return settle(*exchange(o_r, o_p.reshape(2, 4, 8, 1024)))


def solution(mesh):
    split = P("seq", "head")
    out = P(("seq", "head"), None)
    return jax.shard_map(
        on_device, mesh=mesh, in_specs=(split,) * 6 + (P(), P()), out_specs=(out, out), check_vma=False
    )
```
